32 devices in a mesh: patch: 8 (over z, y), hidden: 4 (over x, core).
Axes of the slice: x: 2, y: 2, z: 4, core: 2. Of those that a mesh axis runs over, the one named last changes fastest.
Arguments:
- nodes: bfloat16 [16384, 512], P('patch', 'hidden'), may hold values from -6 to 6
- edges: bfloat16 [65536, 512], P(('patch', 'hidden')), may hold values from -6 to 6
- senders: int32 [65536], P(('patch', 'hidden')), may hold values from 0 to 4159
- receivers: int32 [65536], P(('patch', 'hidden')), may hold values from 0 to 2047
- halo_rows: int32 [8, 2, 1024], P('patch'), may hold values from 0 to 2047
- coarse_rows: int32 [8, 8, 8], P('patch'), may hold values from 0 to 63
- edge_count: int32 [32], P(('patch', 'hidden')), may hold values from 1024 to 2048, as said below
- w_edge_in: bfloat16 [1536, 512], replicated, may hold values from -0.15625 to 0.15625
- b_edge_in: float32 [512], replicated, may hold values from -3 to 3
- w_edge_out: bfloat16 [512, 512], replicated, may hold values from -0.25 to 0.25
- b_edge_out: float32 [512], replicated, may hold values from -2 to 2
- edge_gain: float32 [512], replicated, may hold values from 0.5 to 1.5
- edge_shift: float32 [512], replicated, may hold values from -1 to 1
- w_node_in: bfloat16 [1024, 512], replicated, may hold values from -0.1875 to 0.1875
- b_node_in: float32 [512], replicated, may hold values from -3 to 3
- w_node_out: bfloat16 [512, 512], replicated, may hold values from -0.25 to 0.25
- b_node_out: float32 [512], replicated, may hold values from -2 to 2
- node_gain: float32 [512], replicated, may hold values from 0.5 to 1.5
- node_shift: float32 [512], replicated, may hold values from -1 to 1
Outputs:
- nodes_out: bfloat16 [16384, 512], P('patch', 'hidden')
- edges_out: bfloat16 [65536, 512], P(('patch', 'hidden'))
The draws below stay inside these ranges and needn't reach their ends.
Inputs may be any that keep to these rules, and one draw needn't show every extreme that they name: `edge_count`: some block holds 2048 live edges.
All inputs are finite; a program needn't handle non-finite values.
Results may differ from the reference program's by a relative error of at most 0.007.
Values may be sent and summed in bfloat16 or wider, within the bound.
A program may use at most 128 MiB of HBM per device.

```python
import jax
import jax.numpy as jnp
from jax import lax

D = 512
NODE_DEV = 2048
EDGE_DEV = 2048
COARSE_DEV = 64
SLOT = 8
HALO = 1024
PATCHES = 8
SHARDS = 32
NODES = 16384
EDGES = 65536
TABLE = 4160
N_HIDDEN = 4


def draw_edge_count(key, part):
    draw_key, pick_key = jax.random.split(jax.random.fold_in(key, 11))
    counts = jax.random.randint(draw_key, (SHARDS,), EDGE_DEV // 2, EDGE_DEV + 1)
    busiest = jax.random.randint(pick_key, (), 0, SHARDS)
    return jnp.where(jnp.arange(SHARDS) == busiest, EDGE_DEV, counts).astype(jnp.int32)


def with_ends(result, rng, least, high):
    longest = result.shape.index(max(result.shape))
    spots = []
    for shift in (0, 1):
        where = [jax.random.randint(jax.random.fold_in(rng, axis), (), 0, length) for axis, length in enumerate(result.shape)]
        where[longest] = (where[longest] + shift) % result.shape[longest]
        spots.append(tuple(where))
    return result.at[spots[0]].set(least).at[spots[1]].set(high)


def shard_levels(own_key, dims, shards, least, high):
    def one(dim, parts):
        steps = jax.random.uniform(jax.random.fold_in(jax.random.fold_in(own_key, 6), dim), (parts,), jnp.float32, least / len(shards), high / len(shards))
        return jnp.repeat(jnp.exp(steps), dims[dim] // parts).reshape((-1,) + (1,) * (len(dims) - dim - 1))

    loudness = one(*shards[0])
    for cut in shards[1:]:
        loudness = loudness * one(*cut)
    return loudness


def gaussian(own_key, shape, deviation, most, pieces=(), kind=jnp.bfloat16):
    result = deviation * jax.random.normal(own_key, shape, jnp.float32)
    if pieces:
        result = result * shard_levels(own_key, shape, pieces, -0.22, 0.18)
    return jnp.clip(result, -most, most).astype(kind)


def setup_inputs(seed: int = 0) -> dict:
    seeds = jax.random.split(jax.random.key(seed), 20)
    nodes = gaussian(seeds[0], (NODES, D), 1.0, 6.0, ((0, 8), (1, 4)))
    edges = gaussian(seeds[1], (EDGES, D), 1.0, 6.0, ((0, 32),))
    senders = with_ends(jax.random.randint(seeds[2], (EDGES,), 0, TABLE), jax.random.fold_in(seeds[2], 1), 0, TABLE - 1).astype(jnp.int32)
    receivers = with_ends(jax.random.randint(seeds[3], (EDGES,), 0, NODE_DEV), jax.random.fold_in(seeds[3], 1), 0, NODE_DEV - 1).astype(jnp.int32)
    halo_rows = with_ends(jax.random.randint(seeds[4], (PATCHES, 2, HALO), 0, NODE_DEV), jax.random.fold_in(seeds[4], 1), 0, NODE_DEV - 1).astype(jnp.int32)
    coarse_rows = with_ends(jax.random.randint(seeds[5], (PATCHES, PATCHES, SLOT), 0, COARSE_DEV), jax.random.fold_in(seeds[5], 1), 0, COARSE_DEV - 1).astype(jnp.int32)
    edge_count = draw_edge_count(jax.random.fold_in(seeds[19], 71), 0)
    w_edge_in = gaussian(seeds[7], (3 * D, D), (3 * D) ** -0.5, 0.15625)
    b_edge_in = gaussian(seeds[8], (D,), 0.5, 3.0, (), jnp.float32)
    w_edge_out = gaussian(seeds[9], (D, D), D ** -0.5, 0.25)
    b_edge_out = gaussian(seeds[10], (D,), 0.3, 2.0, (), jnp.float32)
    edge_gain = jnp.clip(1.0 + 0.1 * jax.random.normal(seeds[11], (D,), jnp.float32), 0.5, 1.5)
    edge_shift = gaussian(seeds[12], (D,), 0.2, 1.0, (), jnp.float32)
    w_node_in = gaussian(seeds[13], (2 * D, D), (2 * D) ** -0.5, 0.1875)
    b_node_in = gaussian(seeds[14], (D,), 0.5, 3.0, (), jnp.float32)
    w_node_out = gaussian(seeds[15], (D, D), D ** -0.5, 0.25)
    b_node_out = gaussian(seeds[16], (D,), 0.3, 2.0, (), jnp.float32)
    node_gain = jnp.clip(1.0 + 0.1 * jax.random.normal(seeds[17], (D,), jnp.float32), 0.5, 1.5)
    node_shift = gaussian(seeds[18], (D,), 0.2, 1.0, (), jnp.float32)
    return {"nodes": nodes, "edges": edges, "senders": senders, "receivers": receivers, "halo_rows": halo_rows, "coarse_rows": coarse_rows, "edge_count": edge_count, "w_edge_in": w_edge_in, "b_edge_in": b_edge_in, "w_edge_out": w_edge_out, "b_edge_out": b_edge_out, "edge_gain": edge_gain, "edge_shift": edge_shift, "w_node_in": w_node_in, "b_node_in": b_node_in, "w_node_out": w_node_out, "b_node_out": b_node_out, "node_gain": node_gain, "node_shift": node_shift}


layer_epsilon = 1e-05

def perceptron(inputs, weight_in, bias_in, weight_out, bias_out, norm_gain, norm_shift):
    joined = jnp.concatenate(inputs, axis=1)
    hidden = jnp.dot(joined, weight_in, preferred_element_type=jnp.float32) + bias_in
    active = jax.nn.silu(hidden).astype(jnp.bfloat16)
    output = jnp.dot(active, weight_out, preferred_element_type=jnp.float32) + bias_out
    row_mean = lax.optimization_barrier(jnp.mean(output, axis=1, keepdims=True))
    row_var = lax.optimization_barrier(jnp.mean(jnp.square(output - row_mean), axis=1, keepdims=True))
    return (output - row_mean) * lax.rsqrt(row_var + layer_epsilon) * norm_gain + norm_shift

def block_segments(values, targets):
    return jax.ops.segment_sum(values, targets, num_segments=NODE_DEV)

def reference(nodes, edges, senders, receivers, halo_rows, coarse_rows, edge_count, w_edge_in, b_edge_in, w_edge_out, b_edge_out, edge_gain, edge_shift, w_node_in, b_node_in, w_node_out, b_node_out, node_gain, node_shift):
    patch_edges = N_HIDDEN * EDGE_DEV

    def patch_work(patch_id):
        first_edge = patch_id * patch_edges
        latent = lax.dynamic_slice_in_dim(edges, first_edge, patch_edges, 0)
        sender_code = lax.dynamic_slice_in_dim(senders, first_edge, patch_edges, 0)
        target = lax.dynamic_slice_in_dim(receivers, first_edge, patch_edges, 0)
        counts = lax.dynamic_slice_in_dim(edge_count, patch_id * N_HIDDEN, N_HIDDEN, 0)
        previous = jnp.mod(patch_id - 1, PATCHES).astype(jnp.int32)
        following = jnp.mod(patch_id + 1, PATCHES).astype(jnp.int32)
        from_previous = halo_rows[previous, 1][jnp.clip(sender_code - NODE_DEV, 0, HALO - 1)]
        from_following = halo_rows[following, 0][jnp.clip(sender_code - NODE_DEV - HALO, 0, HALO - 1)]
        far_slot = jnp.clip(sender_code - NODE_DEV - 2 * HALO, 0, PATCHES * SLOT - 1)
        far_owner = far_slot // SLOT
        far_row = coarse_rows[patch_id][far_owner, far_slot % SLOT]
        source = jnp.where(sender_code < NODE_DEV, patch_id * NODE_DEV + sender_code, jnp.where(sender_code < NODE_DEV + HALO, previous * NODE_DEV + from_previous, jnp.where(sender_code < NODE_DEV + 2 * HALO, following * NODE_DEV + from_following, far_owner * NODE_DEV + far_row))).astype(jnp.int32)
        sender_rows = nodes[source]
        patch_nodes = lax.dynamic_slice_in_dim(nodes, patch_id * NODE_DEV, NODE_DEV, 0)
        receiver_rows = patch_nodes[target]
        update = perceptron((latent, sender_rows, receiver_rows), w_edge_in, b_edge_in, w_edge_out, b_edge_out, edge_gain, edge_shift)
        position = jnp.arange(patch_edges, dtype=jnp.int32)
        live_mask = position % EDGE_DEV < counts[position // EDGE_DEV]
        message = jnp.where(live_mask[:, None], update, jnp.zeros_like(update))
        new_latent = (latent.astype(jnp.float32) + message).astype(jnp.bfloat16)
        sent = lax.optimization_barrier(message.astype(jnp.bfloat16)).astype(jnp.float32)
        partial_sums = jax.vmap(block_segments)(sent.reshape(N_HIDDEN, EDGE_DEV, D), target.reshape(N_HIDDEN, EDGE_DEV))
        rounded = lax.optimization_barrier(partial_sums.astype(jnp.bfloat16)).astype(jnp.float32)
        node_sums = lax.optimization_barrier(jnp.sum(rounded, axis=0))
        return (new_latent, node_sums)
    new_edges, node_sums = lax.map(patch_work, jnp.arange(PATCHES, dtype=jnp.int32))
    edges_out = new_edges.reshape(EDGES, D)
    gathered = node_sums.reshape(NODES, D).astype(jnp.bfloat16)
    update = perceptron((nodes, gathered), w_node_in, b_node_in, w_node_out, b_node_out, node_gain, node_shift)
    nodes_out = (nodes.astype(jnp.float32) + update).astype(jnp.bfloat16)
    return (nodes_out, edges_out)
```

```python
import functools

import jax
import jax.numpy as jnp
from jax import lax
from jax.experimental import pallas as pl
from jax.experimental.pallas import tpu as pltpu
from jax.sharding import PartitionSpec as P

layer_epsilon = 1e-05
MESH = pl.DeviceIdType.MESH
f32 = jnp.float32
bf16 = jnp.bfloat16
LANES = 128

PIECES = ((0, 2, "x"), (2, 2, "x"), (4, 1, "x"), (5, 2, "y"), (7, 1, "y"))
NODE_CHUNKS = 4
GATHER = 128


def normalize(output, norm_gain, norm_shift):
    row_mean = jnp.mean(output, axis=1, keepdims=True)
    centered = output - row_mean
    row_var = jnp.mean(jnp.square(centered), axis=1, keepdims=True)
    return centered * lax.rsqrt(row_var + layer_epsilon) * norm_gain + norm_shift


def silu(value):
    half = 0.5 * value
    return half + half * jnp.tanh(half)


def dot(a, b):
    return jnp.dot(a, b, preferred_element_type=f32)


def column_of(row):
    return jnp.transpose(jnp.broadcast_to(row, (LANES, row.shape[1])))[:, :1]


def onehot_of(column, start, count):
    ids = lax.broadcasted_iota(jnp.int32, (column.shape[0], count), 1) + start
    return jnp.where(column == ids, 1.0, 0.0).astype(bf16)


def kernel(
    patches, slot, border, block, quads,
    halo, coarse, live, recv_row,
    b_ei, b_eo, e_gain, e_shift, b_ni, b_no, n_gain, n_shift,
    nodes_hbm, edges_hbm, w_ei_hbm, w_eo_hbm, w_ni_hbm, w_no_hbm, send_hbm, recv_hbm,
    nodes_out, edges,
    table, tab_s, tab_r, got_s, got_r, stage, late_stage, asked, req, rep, far_in, far_out,
    w_ei, w_eo, w_ni, w_no, pre, node_pre, sums_own, msg, send_ids, recv_ids,
    give_far, got_far, give_cross, got_cross, give_near, got_near, fresh,
    load_sem, own_sem, ag_send, ag_recv, halo_send, halo_recv, late_send, late_recv,
    req_send, req_recv, rep_send, rep_recv, rs_send, rs_recv, out_send, out_recv,
):
    p = lax.axis_index("patch")
    h = lax.axis_index("hidden")
    near = h + 1 - 2 * lax.rem(h, 2)
    cross = lax.rem(h + 2, 4)
    diag = lax.rem(near + 2, 4)
    rows, cols = nodes_out.shape
    count, width = edges.shape
    far = patches * slot
    after = lax.rem(p + 1, patches)
    before = lax.rem(p + patches - 1, patches)
    share = rows // 4

    barrier = pltpu.get_barrier_semaphore()
    for step in range(1, patches):
        pl.semaphore_signal(
            barrier, inc=1, device_id={"patch": lax.rem(p + step, patches)}, device_id_type=MESH
        )
    for peer in (near, cross, diag):
        pl.semaphore_signal(barrier, inc=1, device_id={"hidden": peer}, device_id_type=MESH)

    def mine(index):
        return pl.ds(pl.multiple_of(index * cols, cols), cols)

    loads = [
        pltpu.make_async_copy(source, target, load_sem.at[i])
        for i, (source, target) in enumerate((
            (nodes_hbm, table.at[pl.ds(0, rows), mine(h)]),
            (w_ei_hbm, w_ei), (edges_hbm, edges), (recv_hbm, recv_ids), (send_hbm, send_ids),
            (w_ni_hbm, w_ni), (w_eo_hbm, w_eo), (w_no_hbm, w_no),
        ))
    ]
    for load in loads:
        load.start()

    def remote(source, target, s_sem, r_sem, device):
        return pltpu.make_async_remote_copy(
            src_ref=source, dst_ref=target, send_sem=s_sem, recv_sem=r_sem,
            device_id=device, device_id_type=MESH,
        )

    def slots(index):
        return pl.ds(pl.multiple_of(index * slot, slot), slot)

    chunk = rows // NODE_CHUNKS
    spans = [(i * chunk, chunk) for i in range(NODE_CHUNKS)]
    spans.append((rows + 2 * border, far))
    far_span = NODE_CHUNKS
    unit = border // 8
    pieces = []
    for first, units, route in PIECES:
        for side in (1, 0):
            pieces.append((len(spans), side, first * unit, units * unit, route))
            spans.append((rows + (1 - side) * border + first * unit, units * unit))

    def place(k, column):
        start, size = spans[k]
        return table.at[pl.ds(start, size), mine(column)]

    def to_peer(k, j, column, peer, source=None):
        copy = remote(
            place(k, column) if source is None else source, place(k, column),
            ag_send.at[k, j], ag_recv.at[k, j], {"hidden": peer},
        )
        copy.start()
        return copy

    loads[0].wait()
    pl.semaphore_wait(barrier, patches - 1 + 3)

    crossed, neared, passed = {}, {}, {}
    for k in range(NODE_CHUNKS):
        crossed[k] = to_peer(k, 0, h, cross)
        neared[k] = to_peer(k, 1, h, near)

    for owner in range(patches):
        codes = coarse[owner : owner + 1, :].astype(f32)
        square = jnp.broadcast_to(codes, (slot, slot))
        picked = jnp.where(
            lax.broadcasted_iota(jnp.int32, (slot, slot), 0)
            == lax.broadcasted_iota(jnp.int32, (slot, slot), 1), square, 0.0,
        )
        column = jnp.sum(picked, axis=1, keepdims=True)
        asked[pl.ds(owner * slot, slot), :] = jnp.broadcast_to(column, (slot, LANES)).astype(jnp.int32)
    asks = []
    for step in range(1, patches):
        owner = lax.rem(p + step, patches)
        ask = remote(
            asked.at[slots(owner)], req.at[slots(p)],
            req_send.at[step - 1], req_recv.at[step - 1], {"patch": owner},
        )
        ask.start()
        asks.append(ask)
    req[slots(p), :] = asked[slots(p), :]

    def halo_part(side, first, size, column, target):
        ids = column_of(halo[side : side + 1, first : first + size])
        target[...] = dot(onehot_of(ids, 0, rows), table[pl.ds(0, rows), mine(column)]).astype(bf16)

    def halo_copy(source, k, side, column, s_sem, r_sem):
        copy = remote(source, place(k, column), s_sem, r_sem, {"patch": after if side else before})
        copy.start()
        return copy

    halos = {}
    for i, (k, side, first, size, route) in enumerate(pieces):
        held = stage.at[pl.ds(side * border + first, size)]
        halo_part(side, first, size, h, held)
        halos[k] = halo_copy(held, k, side, h, halo_send.at[i], halo_recv.at[i])

    for load in loads[1:3]:
        load.wait()

    def begin(step, carry):
        part = pl.ds(pl.multiple_of(step * block, block), block)
        pre[part, :] = dot(edges[part, :], w_ei[pl.ds(0, width), :]) + b_ei[...]
        return carry

    lax.fori_loop(0, 1, begin, 0)
    for ask in asks:
        ask.wait()
    rep[...] = dot(onehot_of(req[...][:, :1], 0, rows), table[pl.ds(0, rows), mine(h)])
    answers = []
    for step in range(1, patches):
        reader = lax.rem(p + step, patches)
        answer = remote(
            rep.at[slots(reader)], far_in.at[slots(p)],
            rep_send.at[step - 1], rep_recv.at[step - 1], {"patch": reader},
        )
        answer.start()
        answers.append(answer)
    far_in[slots(p), :] = rep[slots(p), :]
    lax.fori_loop(1, count // block, begin, 0)

    def forward(k):
        passed[k] = to_peer(k, 2, cross, near)

    def project(start, size, weight, target):
        projected = dot(table[pl.ds(start, size), :], w_ei[pl.ds(weight * width, width), :])
        for q in range(quads):
            flat = target.reshape(target.shape[0] * quads, LANES)
            flat[pl.ds(start * quads + q, size, stride=quads), :] = (
                projected[:, q * LANES : (q + 1) * LANES]
            )

    def own_chunk(k):
        neared[k].wait()
        passed[k].wait()
        start, size = spans[k]
        project(start, size, 2, tab_r)
        project(start, size, 1, tab_s)

    relayed = [piece for piece in pieces if piece[4] == "x"]
    delayed = [piece for piece in pieces if piece[4] == "y"]

    def relay(piece):
        k = piece[0]
        halos[k].wait()
        if piece[4] == "x":
            crossed[k] = to_peer(k, 0, h, cross)
        neared[k] = to_peer(k, 1, h, near)

    queue = list(relayed)
    for k in range(NODE_CHUNKS):
        crossed[k].wait()
        forward(k)
        if k == 1:
            for answer in answers:
                answer.wait()
            far_out[...] = far_in[...].astype(bf16)
            crossed[far_span] = to_peer(far_span, 0, h, cross, far_out)
            neared[far_span] = to_peer(far_span, 1, h, near, far_out)
            keep = pltpu.make_async_copy(far_out, place(far_span, h), own_sem.at[0])
            keep.start()
        if k == NODE_CHUNKS - 1:
            lates = {}
            for i, (j, side, first, size, route) in enumerate(delayed):
                held = late_stage.at[pl.ds(side * border + first, size)]
                halo_part(side, first, size, cross, held)
                lates[j] = halo_copy(held, j, side, cross, late_send.at[i], late_recv.at[i])
        if k >= 1:
            own_chunk(k - 1)
            for _ in range(2):
                if queue:
                    relay(queue.pop(0))
    while queue:
        relay(queue.pop(0))
    own_chunk(NODE_CHUNKS - 1)
    for piece in delayed:
        relay(piece)
    for load in loads[3:]:
        load.wait()

    def pick(ids, source, target):
        def step(group, carry):
            base = group * GATHER
            for u in range(GATHER):
                target[base + u] = source[ids[base + u]]
            return carry

        lax.fori_loop(0, count // GATHER, step, 0)

    pick(recv_ids, tab_r, got_r)
    own_rows = pl.ds(pl.multiple_of(h * share, share), share)
    node_pre[...] = dot(table[own_rows, :], w_ni[pl.ds(0, width), :]) + b_ni[...]

    keep.wait()
    crossed[far_span].wait()
    forward(far_span)
    for piece in relayed:
        crossed[piece[0]].wait()
        forward(piece[0])
    neared[far_span].wait()
    passed[far_span].wait()
    project(spans[far_span][0], spans[far_span][1], 1, tab_s)
    for piece in relayed:
        k = piece[0]
        neared[k].wait()
        passed[k].wait()
        project(spans[k][0], spans[k][1], 1, tab_s)
    for piece in delayed:
        lates[piece[0]].wait()
        forward(piece[0])
    for piece in delayed:
        k = piece[0]
        neared[k].wait()
        passed[k].wait()
        project(spans[k][0], spans[k][1], 1, tab_s)

    pick(send_ids, tab_s, got_s)

    def edge(step, carry):
        base = pl.multiple_of(step * block, block)
        part = pl.ds(base, block)
        total = [
            pre[part, q * LANES : (q + 1) * LANES]
            + got_r.reshape(count * quads, LANES)[pl.ds(base * quads + q, block, stride=quads), :]
            + got_s.reshape(count * quads, LANES)[pl.ds(base * quads + q, block, stride=quads), :]
            for q in range(quads)
        ]
        active = silu(jnp.concatenate(total, axis=1)).astype(bf16)
        output = dot(active, w_eo[...]) + b_eo[...]
        update = normalize(output, e_gain[...], e_shift[...])
        position = lax.broadcasted_iota(jnp.int32, (block, 1), 0) + step * block
        message = jnp.where(position < live[0], update, 0.0)
        msg[part, :] = message.astype(bf16)
        edges[part, :] = (edges[part, :].astype(f32) + message).astype(bf16)
        return carry

    lax.fori_loop(0, count // block, edge, 0)

    half = share // 2

    def sums(owner, c):
        ids = lax.broadcasted_iota(jnp.int32, (half, count), 0) + (owner * share + c * half)
        return dot(jnp.where(recv_row[...] == ids, 1.0, 0.0).astype(bf16), msg[...])

    to_far, to_near, to_cross = [], [], []
    for c in range(2):
        part = pl.ds(c * half, half)
        give_far[part, :] = sums(diag, c).astype(bf16)
        copy = remote(
            give_far.at[part], got_far.at[part], rs_send.at[c], rs_recv.at[c], {"hidden": near}
        )
        copy.start()
        to_far.append(copy)
    cut = share // 4
    for c in range(2):
        part = pl.ds(c * half, half)
        total = sums(cross, c)
        to_far[c].wait()
        give_cross[part, :] = (total + got_far[part, :].astype(f32)).astype(bf16)
        for i in (2 * c, 2 * c + 1):
            piece = pl.ds(i * cut, cut)
            copy = remote(
                give_cross.at[piece], got_cross.at[piece], rs_send.at[2 + i], rs_recv.at[2 + i],
                {"hidden": cross},
            )
            copy.start()
            to_cross.append(copy)
    for c in range(2):
        part = pl.ds(c * half, half)
        give_near[part, :] = sums(near, c).astype(bf16)
        copy = remote(
            give_near.at[part], got_near.at[part], rs_send.at[6 + c], rs_recv.at[6 + c], {"hidden": near}
        )
        copy.start()
        to_near.append(copy)
    for c in range(2):
        sums_own[pl.ds(c * half, half), :] = sums(h, c)
    for copy in to_near:
        copy.wait()
    outs = []
    for i in range(4):
        part = pl.ds(i * cut, cut)
        to_cross[i].wait()
        total = sums_own[part, :] + got_near[part, :].astype(f32) + got_cross[part, :].astype(f32)
        inner = node_pre[part, :] + dot(total.astype(bf16), w_ni[pl.ds(width, width), :])
        output = dot(silu(inner).astype(bf16), w_no[...]) + b_no[...]
        update = normalize(output, n_gain[...], n_shift[...])
        spot = pl.ds(pl.multiple_of(h * share + i * cut, cut), cut)
        fresh[part, :] = (table[spot, :].astype(f32) + update).astype(bf16)
        for j, peer in enumerate((cross, diag, near)):
            copy = remote(
                fresh.at[part, mine(peer)], nodes_out.at[spot, :],
                out_send.at[i, j], out_recv.at[i, j], {"hidden": peer},
            )
            copy.start()
            outs.append(copy)
        nodes_out[spot, :] = fresh[part, mine(h)]
    for copy in outs:
        copy.wait()


def local(
    nodes, edges, senders, receivers, halo_rows, coarse_rows, edge_count,
    w_edge_in, b_edge_in, w_edge_out, b_edge_out, edge_gain, edge_shift,
    w_node_in, b_node_in, w_node_out, b_node_out, node_gain, node_shift,
    *, patches,
):
    rows, cols = nodes.shape
    count, width = edges.shape
    border = halo_rows.shape[2]
    slot = coarse_rows.shape[2]
    far = patches * slot
    table_rows = rows + 2 * border + far
    share = rows // 4
    block = min(512, count)
    quads = width // LANES
    vmem = pl.BlockSpec(memory_space=pltpu.VMEM)
    smem = pl.BlockSpec(memory_space=pltpu.SMEM)
    hbm = pl.BlockSpec(memory_space=pl.ANY)
    dma = pltpu.SemaphoreType.DMA
    spans = NODE_CHUNKS + 1 + 2 * len(PIECES)
    late = 2 * sum(piece[2] == "y" for piece in PIECES)
    return pl.pallas_call(
        functools.partial(kernel, patches, slot, border, block, quads),
        out_shape=(pltpu.VMEM((rows, cols), bf16), pltpu.VMEM((count, width), bf16)),
        in_specs=[vmem] * 2 + [smem] + [vmem] * 9 + [hbm] * 8,
        out_specs=(vmem, vmem),
        scratch_shapes=[
            pltpu.VMEM((table_rows, width), bf16),
            pltpu.VMEM((table_rows, quads, LANES), f32),
            pltpu.VMEM((rows, quads, LANES), f32),
            pltpu.VMEM((count, quads, LANES), f32),
            pltpu.VMEM((count, quads, LANES), f32),
            pltpu.VMEM((2 * border, cols), bf16),
            pltpu.VMEM((2 * border, cols), bf16),
            pltpu.VMEM((far, LANES), jnp.int32),
            pltpu.VMEM((far, LANES), jnp.int32),
            pltpu.VMEM((far, cols), f32),
            pltpu.VMEM((far, cols), f32),
            pltpu.VMEM((far, cols), bf16),
            pltpu.VMEM(w_edge_in.shape, bf16),
            pltpu.VMEM(w_edge_out.shape, bf16),
            pltpu.VMEM(w_node_in.shape, bf16),
            pltpu.VMEM(w_node_out.shape, bf16),
            pltpu.VMEM((count, width), f32),
            pltpu.VMEM((share, width), f32),
            pltpu.VMEM((share, width), f32),
            pltpu.VMEM((count, width), bf16),
            pltpu.SMEM((count,), jnp.int32),
            pltpu.SMEM((count,), jnp.int32),
        ] + [pltpu.VMEM((share, width), bf16)] * 7 + [
            dma((8,)), dma((1,)), dma((spans, 3)), dma((spans, 3)),
            dma((2 * len(PIECES),)), dma((2 * len(PIECES),)), dma((late,)), dma((late,)),
            dma((patches - 1,)), dma((patches - 1,)), dma((patches - 1,)), dma((patches - 1,)),
            dma((8,)), dma((8,)), dma((4, 3)), dma((4, 3)),
        ],
        compiler_params=pltpu.CompilerParams(
            collective_id=0, has_side_effects=True, vmem_limit_bytes=56 * 1024 * 1024
        ),
    )(
        halo_rows.reshape(2, border), coarse_rows.reshape(patches, slot), edge_count,
        receivers.reshape(1, -1),
        b_edge_in.reshape(1, -1), b_edge_out.reshape(1, -1),
        edge_gain.reshape(1, -1), edge_shift.reshape(1, -1),
        b_node_in.reshape(1, -1), b_node_out.reshape(1, -1),
        node_gain.reshape(1, -1), node_shift.reshape(1, -1),
        nodes, edges, w_edge_in, w_edge_out, w_node_in, w_node_out, senders, receivers,
    )


def solution(mesh):
    spread = P(("patch", "hidden"))
    return jax.shard_map(
        functools.partial(local, patches=mesh.shape["patch"]),
        mesh=mesh,
        in_specs=(
            P("patch", "hidden"), P(("patch", "hidden"), None), spread, spread,
            P("patch", None, None), P("patch", None, None), spread,
        ) + (P(),) * 12,
        out_specs=(P("patch", "hidden"), P(("patch", "hidden"), None)),
        check_vma=False,
    )
```

```python
import functools

import jax
import jax.numpy as jnp
from jax import lax
from jax.experimental import pallas as pl
from jax.experimental.pallas import tpu as pltpu
from jax.sharding import PartitionSpec as P

layer_epsilon = 1e-05
MESH = pl.DeviceIdType.MESH
f32 = jnp.float32
bf16 = jnp.bfloat16
LANES = 128

PIECES = ((0, 2, "x"), (2, 2, "x"), (4, 1, "x"), (5, 1, "y"), (6, 2, "y"))
NODE_CHUNKS = 4
GATHER = 128
STORE_PARTS = 4


def normalize(output, norm_gain, norm_shift):
    row_mean = jnp.mean(output, axis=1, keepdims=True)
    centered = output - row_mean
    row_var = jnp.mean(jnp.square(centered), axis=1, keepdims=True)
    return centered * lax.rsqrt(row_var + layer_epsilon) * norm_gain + norm_shift


def silu_of_half(half):
    return half + half * jnp.tanh(half)


def dot(a, b):
    return jnp.dot(a, b, preferred_element_type=f32)


def onehot_of(column, start, count):
    ids = lax.broadcasted_iota(jnp.int32, (column.shape[0], count), 1) + start
    return jnp.where(column == ids, 1.0, 0.0).astype(bf16)


def kernel(
    patches, slot, border, block, quads,
    nodes_hbm, halo_hbm, coarse_hbm, edges_hbm, w_ei_hbm, w_eo_hbm, w_ni_hbm, w_no_hbm,
    send_hbm, recv_hbm, recv_row_hbm, live_hbm, *rest,
):
    vectors_hbm = rest[:8]
    (
        nodes_out, edges,
        table, tab_s, tab_r, got_s0, got_s1, got_r, plain, picked_rows, stage, late_stage,
        coarse, asked, req, rep, far_in, far_out, recv_row, vectors,
        w_ei, w_eo, w_ni, w_no, pre, node_pre, sums_own, msg,
        send_ids, recv_ids, halo_ids, live,
        give_far, got_far, give_cross, got_cross, give_near, got_near, fresh,
        load_sem, own_sem, ag_send, cross_recv, pass_recv, halo_send, halo_recv, late_send, late_recv,
        ask_sem, rs_send, rs_recv, out_sem,
    ) = rest[8:]
    got_s = (got_s0, got_s1)
    b_ei, b_eo, e_gain, e_shift, b_ni, b_no, n_gain, n_shift = [vectors.at[i] for i in range(8)]
    p = lax.axis_index("patch")
    h = lax.axis_index("hidden")
    near = h + 1 - 2 * lax.rem(h, 2)
    cross = lax.rem(h + 2, 4)
    diag = lax.rem(near + 2, 4)
    rows, cols = nodes_out.shape
    count, width = edges.shape
    far = patches * slot
    after = lax.rem(p + 1, patches)
    before = lax.rem(p + patches - 1, patches)
    share = rows // 4

    barrier = pltpu.get_barrier_semaphore()
    for step in range(1, patches):
        pl.semaphore_signal(
            barrier, inc=1, device_id={"patch": lax.rem(p + step, patches)}, device_id_type=MESH
        )
    for peer in (near, cross, diag):
        pl.semaphore_signal(barrier, inc=1, device_id={"hidden": peer}, device_id_type=MESH)

    def mine(index):
        return pl.ds(pl.multiple_of(index * cols, cols), cols)

    def load(i, *pairs):
        copies = [pltpu.make_async_copy(source, target, load_sem.at[i]) for source, target in pairs]
        for copy in copies:
            copy.start()
        return copies[0]

    load_nodes = load(0, (nodes_hbm, table.at[pl.ds(0, rows), mine(h)]))
    border_ids = [halo_ids.at[pl.ds(side * border, border)] for side in range(2)]
    load_halo = [load((11, 1)[side], (halo_hbm.at[side], border_ids[side])) for side in range(2)]
    load_coarse = load(2, (coarse_hbm, coarse))
    load_edges = load(3, (edges_hbm, edges))
    load_in = load(4, (w_ei_hbm, w_ei))
    load(5, *[(source, vectors.at[i]) for i, source in enumerate(vectors_hbm)])
    load_recv = load(6, (recv_hbm, recv_ids))
    load_send = load(7, (send_hbm, send_ids))
    load_row = load(8, (recv_row_hbm, recv_row))
    load_live = load(9, (live_hbm, live))
    load(10, (w_ni_hbm, w_ni), (w_eo_hbm, w_eo), (w_no_hbm, w_no))

    def remote(source, target, s_sem, r_sem, device):
        return pltpu.make_async_remote_copy(
            src_ref=source, dst_ref=target, send_sem=s_sem, recv_sem=r_sem,
            device_id=device, device_id_type=MESH,
        )

    def slots(index):
        return pl.ds(pl.multiple_of(index * slot, slot), slot)

    def drain(sem, blocks, sent=False):
        ref = table.at[pl.ds(0, blocks // quads)]
        total = remote(ref, ref, sem, sem, {"hidden": near})
        if sent:
            total.wait_send()
        else:
            total.wait_recv()

    chunk = rows // NODE_CHUNKS
    spans = [(i * chunk, chunk) for i in range(NODE_CHUNKS)]
    spans.append((rows + 2 * border, far))
    far_span = NODE_CHUNKS
    unit = border // 8
    pieces = []
    for first, units, route in PIECES:
        for side in (1, 0):
            pieces.append((len(spans), side, first * unit, units * unit, route))
            spans.append((rows + (1 - side) * border + first * unit, units * unit))
    early_group, late_group = NODE_CHUNKS, NODE_CHUNKS + 1
    group = {k: k for k in range(NODE_CHUNKS)}
    group[far_span] = late_group
    for k, side, first, size, route in pieces:
        group[k] = early_group if first + size <= border // 2 else late_group
    sent_rows = [0, 0]
    group_rows = [0] * (NODE_CHUNKS + 2)

    def place(k, column):
        start, size = spans[k]
        return table.at[pl.ds(start, size), mine(column)]

    def to_peer(k, j, column, peer, source=None):
        kind = 0 if k < NODE_CHUNKS else 1
        sent_rows[kind] += spans[k][1]
        if j:
            group_rows[group[k]] += spans[k][1]
        copy = remote(
            place(k, column) if source is None else source, place(k, column),
            ag_send.at[kind], pass_recv.at[group[k]] if j else cross_recv.at[k], {"hidden": peer},
        )
        copy.start()
        return copy

    load_nodes.wait()
    pl.semaphore_wait(barrier, patches - 1 + 3)

    crossed = {}
    for k in range(NODE_CHUNKS):
        crossed[k] = to_peer(k, 0, h, cross)
        to_peer(k, 1, h, near)

    load_coarse.wait()
    for owner in range(patches):
        codes = coarse[owner : owner + 1, :].astype(f32)
        square = jnp.broadcast_to(codes, (slot, slot))
        picked = jnp.where(
            lax.broadcasted_iota(jnp.int32, (slot, slot), 0)
            == lax.broadcasted_iota(jnp.int32, (slot, slot), 1), square, 0.0,
        )
        column = jnp.sum(picked, axis=1, keepdims=True)
        asked[pl.ds(owner * slot, slot), :] = jnp.broadcast_to(column, (slot, LANES)).astype(jnp.int32)
    for step in range(1, patches):
        owner = lax.rem(p + step, patches)
        remote(
            asked.at[slots(owner)], req.at[slots(p)], ask_sem.at[0], ask_sem.at[1], {"patch": owner}
        ).start()
    req[slots(p), :] = asked[slots(p), :]
    others = pl.ds(0, (patches - 1) * slot)

    def spread(column):
        plain.reshape(rows, LANES)[...] = table[pl.ds(0, rows), mine(column)].astype(f32)

    def choose(first, size):
        def step(part, carry):
            base = first + part * GATHER
            for u in range(GATHER):
                picked_rows[base + u] = plain[halo_ids[base + u]]
            return carry

        lax.fori_loop(0, size // GATHER, step, 0)

    def halo_part(target, side, first, size):
        start = side * border + first
        choose(start, size)
        part = pl.ds(start, size)
        target[part, :] = picked_rows.reshape(2 * border, LANES)[part, :].astype(bf16)
        return target.at[part]

    def halo_copy(source, k, side, column, s_sem, r_sem):
        copy = remote(source, place(k, column), s_sem, r_sem, {"patch": after if side else before})
        copy.start()
        return copy

    relayed = [piece for piece in pieces if piece[4] == "x"]
    delayed = [piece for piece in pieces if piece[4] == "y"]
    for side in range(2):
        load_halo[side].wait()
    spread(h)
    halos = {}

    def send_halo(i, piece):
        k, side, first, size, route = piece
        held = halo_part(stage, side, first, size)
        halos[k] = halo_copy(held, k, side, h, halo_send.at[0], halo_recv.at[min(i, len(relayed))])

    for i, piece in enumerate(relayed):
        send_halo(i, piece)
    asks = remote(asked.at[others], req.at[others], ask_sem.at[0], ask_sem.at[1], {"hidden": near})
    asks.wait()
    rep[...] = dot(onehot_of(req[...][:, :1], 0, rows), table[pl.ds(0, rows), mine(h)])
    for step in range(1, patches):
        reader = lax.rem(p + step, patches)
        remote(
            rep.at[slots(reader)], far_in.at[slots(p)], ask_sem.at[2], ask_sem.at[3], {"patch": reader}
        ).start()
    answers = remote(rep.at[others], far_in.at[others], ask_sem.at[2], ask_sem.at[3], {"hidden": near})
    far_in[slots(p), :] = rep[slots(p), :]
    for i, piece in enumerate(delayed):
        send_halo(len(relayed) + i, piece)

    load_edges.wait()
    load_in.wait()
    remote(vectors, vectors, load_sem.at[5], load_sem.at[5], {"hidden": near}).wait_recv()

    def begin(step, carry):
        part = pl.ds(pl.multiple_of(step * block, block), block)
        pre[part, :] = 0.5 * (dot(edges[part, :], w_ei[pl.ds(0, width), :]) + b_ei[...])
        return carry

    lax.fori_loop(0, count // block, begin, 0)

    def forward(k):
        to_peer(k, 2, cross, near)

    def project(start, size, weight, target):
        projected = 0.5 * dot(table[pl.ds(start, size), :], w_ei[pl.ds(weight * width, width), :])
        flat = target.reshape(target.shape[0] * quads, LANES)
        for q in range(quads):
            flat[pl.ds(start * quads + q, size, stride=quads), :] = (
                projected[:, q * LANES : (q + 1) * LANES]
            )

    def own_chunk(k):
        drain(pass_recv.at[k], group_rows[k])
        start, size = spans[k]
        project(start, size, 2, tab_r)
        project(start, size, 1, tab_s)

    def relay(piece):
        k = piece[0]
        halos[k].wait_recv()
        crossed[k] = to_peer(k, 0, h, cross)
        to_peer(k, 1, h, near)

    queue = list(relayed)
    for k in range(NODE_CHUNKS):
        crossed[k].wait_recv()
        forward(k)
        if k == NODE_CHUNKS - 1:
            while queue:
                relay(queue.pop(0))
            spread(cross)
            lates = []
            for i, (j, side, first, size, route) in enumerate(delayed):
                held = halo_part(late_stage, side, first, size)
                lates.append((j, halo_copy(held, j, side, cross, late_send.at[0], late_recv.at[i])))
            answers.wait()
            far_out[...] = far_in[...].astype(bf16)
            crossed[far_span] = to_peer(far_span, 0, h, cross, far_out)
            to_peer(far_span, 1, h, near, far_out)
            keep = pltpu.make_async_copy(far_out, place(far_span, h), own_sem.at[0])
            keep.start()
        if k >= 1:
            for _ in range(2):
                if queue:
                    relay(queue.pop(0))
            own_chunk(k - 1)
    own_chunk(NODE_CHUNKS - 1)
    late_rows = sum(piece[3] for piece in delayed)
    drain(halo_recv.at[len(relayed)], late_rows)
    for piece in delayed:
        to_peer(piece[0], 1, h, near)
    load_recv.wait()
    load_send.wait()

    def pick_receivers(start, size):
        def step(part, carry):
            base = start + part * GATHER
            for u in range(GATHER):
                got_r[base + u] = tab_r[recv_ids[base + u]]
            return carry

        lax.fori_loop(0, size // GATHER, step, 0)

    early = [piece for piece in relayed if group[piece[0]] == early_group]
    parts = max(1, len(early) // 2)
    keep.wait()
    for i in range(parts):
        pick_receivers(i * (count // parts), count // parts)
        for piece in early[2 * i : 2 * i + 2]:
            crossed[piece[0]].wait_recv()
            forward(piece[0])

    def merge(step, carry):
        part = pl.ds(pl.multiple_of(step * block, block), block)
        wide = got_r.reshape(count * quads, LANES)
        for q in range(quads):
            lanes = pl.ds(q * LANES, LANES)
            pre[part, lanes] = (
                pre[part, lanes] + wide[pl.ds(step * block * quads + q, block, stride=quads), :]
            )
        return carry

    lax.fori_loop(0, count // block, merge, 0)
    drain(load_sem.at[10], 4 * width * quads)
    own_rows = pl.ds(pl.multiple_of(h * share, share), share)
    node_pre[...] = dot(table[own_rows, :], w_ni[pl.ds(0, width), :]) + b_ni[...]
    drain(pass_recv.at[early_group], group_rows[early_group])
    for side in range(2):
        project(rows + side * border, border // 2, 1, tab_s)
    for piece in relayed:
        if group[piece[0]] == late_group:
            crossed[piece[0]].wait_recv()
            forward(piece[0])
    crossed[far_span].wait_recv()
    forward(far_span)
    for j, copy in lates:
        copy.wait_recv()
        forward(j)
    drain(pass_recv.at[late_group], group_rows[late_group])
    project(spans[far_span][0], spans[far_span][1], 1, tab_s)
    for side in range(2):
        project(rows + side * border + border // 2, border // 2, 1, tab_s)
    load_live.wait()
    load_row.wait()

    def pick_block(index, first, size):
        for u in range(first, first + size):
            got_s[index % 2][u] = tab_s[send_ids[index * block + u]]

    def pick_first(step, carry):
        for u in range(GATHER):
            got_s[0][step * GATHER + u] = tab_s[send_ids[step * GATHER + u]]
        return carry

    def edge(index):
        part = pl.ds(index * block, block)
        wide_s = got_s[index % 2].reshape(block * quads, LANES)
        total = [
            pre[part, q * LANES : (q + 1) * LANES]
            + wide_s[pl.ds(q, block, stride=quads), :]
            for q in range(quads)
        ]
        active = silu_of_half(jnp.concatenate(total, axis=1)).astype(bf16)
        output = dot(active, w_eo[...]) + b_eo[...]
        update = normalize(output, e_gain[...], e_shift[...])
        position = lax.broadcasted_iota(jnp.int32, (block, 1), 0) + index * block
        message = jnp.where(position < live[0], update, 0.0)
        msg[part, :] = message.astype(bf16)
        edges[part, :] = (edges[part, :].astype(f32) + message).astype(bf16)

    lax.fori_loop(0, block // GATHER, pick_first, 0)
    for index in range(count // block):
        if index + 1 < count // block:
            pick_block(index + 1, 0, block)
        edge(index)

    cut = share // 4

    def sums(owner, first, size):
        ids = lax.broadcasted_iota(jnp.int32, (size, count), 0) + (owner * share + first)
        return dot(jnp.where(recv_row[...] == ids, 1.0, 0.0).astype(bf16), msg[...])

    def give_sums(owner, first, size, target, source, r_sem):
        part = pl.ds(first, size)
        source[part, :] = sums(owner, first, size).astype(bf16)
        copy = remote(source.at[part], target.at[part], rs_send.at[0], r_sem, {"hidden": near})
        copy.start()
        return copy

    to_cross = []

    def cross_sums(first, size, copy):
        part = pl.ds(first, size)
        total = sums(cross, first, size)
        copy.wait_recv()
        give_cross[part, :] = (total + got_far[part, :].astype(f32)).astype(bf16)
        for i in range(first // cut, (first + size) // cut):
            piece = pl.ds(i * cut, cut)
            copy = remote(
                give_cross.at[piece], got_cross.at[piece], rs_send.at[0], rs_recv.at[4 + i],
                {"hidden": cross},
            )
            copy.start()
            to_cross.append(copy)

    parts = ((0, cut), (cut, cut), (2 * cut, share - 2 * cut))
    begun = [
        give_sums(diag, *parts[i], got_far, give_far, rs_recv.at[i]) for i in range(2)
    ]
    cross_sums(*parts[0], begun[0])
    cross_sums(*parts[1], begun[1])
    begun.append(give_sums(diag, *parts[2], got_far, give_far, rs_recv.at[2]))
    cross_sums(*parts[2], begun[2])
    to_near = give_sums(near, 0, share, got_near, give_near, rs_recv.at[3])
    sums_own[...] = sums(h, 0, share)
    to_near.wait_recv()
    for i in range(4):
        part = pl.ds(i * cut, cut)
        to_cross[i].wait_recv()
        total = sums_own[part, :] + got_near[part, :].astype(f32) + got_cross[part, :].astype(f32)
        inner = node_pre[part, :] + dot(total.astype(bf16), w_ni[pl.ds(width, width), :])
        output = dot(silu_of_half(0.5 * inner).astype(bf16), w_no[...]) + b_no[...]
        update = normalize(output, n_gain[...], n_shift[...])
        spot = pl.ds(pl.multiple_of(h * share + i * cut, cut), cut)
        fresh[part, :] = (table[spot, :].astype(f32) + update).astype(bf16)
        for peer in (cross, diag, near):
            remote(
                fresh.at[part, mine(peer)], nodes_out.at[spot, :],
                out_sem.at[0], out_sem.at[1], {"hidden": peer},
            ).start()
        nodes_out[spot, :] = fresh[part, mine(h)]
    for kind in range(2):
        drain(ag_send.at[kind], sent_rows[kind], True)
    drain(halo_send.at[0], 2 * border, True)
    drain(late_send.at[0], late_rows, True)
    drain(rs_send.at[0], 3 * share * quads, True)
    drain(out_sem.at[0], 3 * share, True)
    drain(out_sem.at[1], 3 * share)


def store(nodes, edges, nodes_out, edges_out, sems):
    size = edges.shape[0] // STORE_PARTS
    copies = [
        pltpu.make_async_copy(
            edges.at[pl.ds(i * size, size)], edges_out.at[pl.ds(i * size, size)], sems.at[i]
        )
        for i in range(STORE_PARTS)
    ]
    copies.append(pltpu.make_async_copy(nodes, nodes_out, sems.at[STORE_PARTS]))
    for copy in copies:
        copy.start()
    for copy in copies:
        copy.wait()


def local(
    nodes, edges, senders, receivers, halo_rows, coarse_rows, edge_count,
    w_edge_in, b_edge_in, w_edge_out, b_edge_out, edge_gain, edge_shift,
    w_node_in, b_node_in, w_node_out, b_node_out, node_gain, node_shift,
    *, patches,
):
    rows, cols = nodes.shape
    count, width = edges.shape
    border = halo_rows.shape[2]
    slot = coarse_rows.shape[2]
    far = patches * slot
    table_rows = rows + 2 * border + far
    share = rows // 4
    block = min(512, count)
    quads = width // LANES
    vmem = pl.BlockSpec(memory_space=pltpu.VMEM)
    hbm = pl.BlockSpec(memory_space=pl.ANY)
    dma = pltpu.SemaphoreType.DMA
    spans = NODE_CHUNKS + 1 + 2 * len(PIECES)
    late = 2 * sum(piece[2] == "y" for piece in PIECES)
    i32 = jnp.int32
    fresh_nodes, fresh_edges = pl.pallas_call(
        functools.partial(kernel, patches, slot, border, block, quads),
        out_shape=(pltpu.VMEM((rows, cols), bf16), pltpu.VMEM((count, width), bf16)),
        in_specs=[hbm] * 20,
        out_specs=(vmem, vmem),
        scratch_shapes=[
            pltpu.VMEM((table_rows, width), bf16),
            pltpu.VMEM((table_rows, quads, LANES), f32),
            pltpu.VMEM((rows, quads, LANES), f32),
            pltpu.VMEM((block, quads, LANES), f32),
            pltpu.VMEM((block, quads, LANES), f32),
            pltpu.VMEM((count, quads, LANES), f32),
            pltpu.VMEM((rows, 1, LANES), f32),
            pltpu.VMEM((2 * border, 1, LANES), f32),
            pltpu.VMEM((2 * border, cols), bf16),
            pltpu.VMEM((2 * border, cols), bf16),
            pltpu.VMEM((patches, slot), i32),
            pltpu.VMEM((far, LANES), i32),
            pltpu.VMEM((far, LANES), i32),
            pltpu.VMEM((far, cols), f32),
            pltpu.VMEM((far, cols), f32),
            pltpu.VMEM((far, cols), bf16),
            pltpu.VMEM((1, count), i32),
            pltpu.VMEM((8, 1, width), f32),
            pltpu.VMEM(w_edge_in.shape, bf16),
            pltpu.VMEM(w_edge_out.shape, bf16),
            pltpu.VMEM(w_node_in.shape, bf16),
            pltpu.VMEM(w_node_out.shape, bf16),
            pltpu.VMEM((count, width), f32),
            pltpu.VMEM((share, width), f32),
            pltpu.VMEM((share, width), f32),
            pltpu.VMEM((count, width), bf16),
            pltpu.SMEM((count,), i32),
            pltpu.SMEM((count,), i32),
            pltpu.SMEM((2 * border,), i32),
            pltpu.SMEM((1,), i32),
        ] + [pltpu.VMEM((share, width), bf16)] * 7 + [
            dma((12,)), dma((1,)), dma((2,)), dma((spans - late,)), dma((NODE_CHUNKS + 2,)),
            dma((1,)), dma((2 * len(PIECES) - late + 1,)), dma((1,)), dma((late,)),
            dma((4,)), dma((1,)), dma((8,)), dma((2,)),
        ],
        compiler_params=pltpu.CompilerParams(
            collective_id=0, has_side_effects=True, vmem_limit_bytes=56 * 1024 * 1024
        ),
    )(
        nodes, halo_rows.reshape(2, border), coarse_rows.reshape(patches, slot),
        edges, w_edge_in, w_edge_out, w_node_in, w_node_out, senders, receivers,
        receivers.reshape(1, -1), edge_count,
        b_edge_in.reshape(1, -1), b_edge_out.reshape(1, -1),
        edge_gain.reshape(1, -1), edge_shift.reshape(1, -1),
        b_node_in.reshape(1, -1), b_node_out.reshape(1, -1),
        node_gain.reshape(1, -1), node_shift.reshape(1, -1),
    )
    return pl.pallas_call(
        store,
        out_shape=(
            jax.ShapeDtypeStruct((rows, cols), bf16), jax.ShapeDtypeStruct((count, width), bf16)
        ),
        in_specs=[vmem] * 2,
        out_specs=(hbm, hbm),
        scratch_shapes=[dma((1 + STORE_PARTS,))],
    )(
        pltpu.with_memory_space_constraint(fresh_nodes, pltpu.VMEM),
        pltpu.with_memory_space_constraint(fresh_edges, pltpu.VMEM),
    )


def solution(mesh):
    spread = P(("patch", "hidden"))
    return jax.shard_map(
        functools.partial(local, patches=mesh.shape["patch"]),
        mesh=mesh,
        in_specs=(
            P("patch", "hidden"), P(("patch", "hidden"), None), spread, spread,
            P("patch", None, None), P("patch", None, None), spread,
        ) + (P(),) * 12,
        out_specs=(P("patch", "hidden"), P(("patch", "hidden"), None)),
        check_vma=False,
    )
```

```python
import functools

import jax
import jax.numpy as jnp
from jax import lax
from jax.experimental import pallas as pl
from jax.experimental.pallas import tpu as pltpu
from jax.sharding import PartitionSpec as P

layer_epsilon = 1e-05
MESH = pl.DeviceIdType.MESH
f32 = jnp.float32
bf16 = jnp.bfloat16
LANES = 128

PIECES = ((0, 2, "x"), (2, 2, "x"), (4, 2, "y"), (6, 2, "y"))
NODE_CHUNKS = 4
GATHER = 128
STORE_PARTS = 4


def normalize(output, norm_gain, norm_shift):
    row_mean = jnp.mean(output, axis=1, keepdims=True)
    centered = output - row_mean
    row_var = jnp.mean(jnp.square(centered), axis=1, keepdims=True)
    return centered * lax.rsqrt(row_var + layer_epsilon) * norm_gain + norm_shift


def silu_of_half(half):
    return half + half * jnp.tanh(half)


def dot(a, b):
    return jnp.dot(a, b, preferred_element_type=f32)


def onehot_of(column, start, count):
    ids = lax.broadcasted_iota(jnp.int32, (column.shape[0], count), 1) + start
    return jnp.where(column == ids, 1.0, 0.0).astype(bf16)


def kernel(
    patches, slot, border, block, quads,
    nodes_hbm, halo_hbm, coarse_hbm, edges_hbm, w_ei_hbm, w_eo_hbm, w_ni_hbm, w_no_hbm,
    send_hbm, recv_hbm, recv_row_hbm, live_hbm, *rest,
):
    vectors_hbm = rest[:8]
    (
        nodes_out, edges,
        table, tab_s, tab_r, got_s0, got_s1, got_r, plain, picked_rows, stage, late_stage,
        coarse, asked, req, rep, far_in, far_out, recv_row, vectors,
        w_ei, w_eo, w_ni, w_no, pre, node_pre, sums_own, msg,
        send_ids, recv_ids, halo_ids, live,
        give_far, got_far, give_cross, got_cross, give_near, got_near, fresh,
        load_sem, own_sem, ag_send, cross_recv, pass_recv, halo_send, halo_recv, late_send, late_recv,
        ask_sem, rs_send, rs_recv, out_sem,
    ) = rest[8:]
    got_s = (got_s0, got_s1)
    b_ei, b_eo, e_gain, e_shift, b_ni, b_no, n_gain, n_shift = [vectors.at[i] for i in range(8)]
    p = lax.axis_index("patch")
    h = lax.axis_index("hidden")
    near = h + 1 - 2 * lax.rem(h, 2)
    cross = lax.rem(h + 2, 4)
    diag = lax.rem(near + 2, 4)
    rows, cols = nodes_out.shape
    count, width = edges.shape
    far = patches * slot
    after = lax.rem(p + 1, patches)
    before = lax.rem(p + patches - 1, patches)
    share = rows // 4

    barrier = pltpu.get_barrier_semaphore()
    for step in range(1, patches):
        pl.semaphore_signal(
            barrier, inc=1, device_id={"patch": lax.rem(p + step, patches)}, device_id_type=MESH
        )
    for peer in (near, cross, diag):
        pl.semaphore_signal(barrier, inc=1, device_id={"hidden": peer}, device_id_type=MESH)

    def mine(index):
        return pl.ds(pl.multiple_of(index * cols, cols), cols)

    def load(i, *pairs):
        copies = [pltpu.make_async_copy(source, target, load_sem.at[i]) for source, target in pairs]
        for copy in copies:
            copy.start()
        return copies[0]

    load_nodes = load(0, (nodes_hbm, table.at[pl.ds(0, rows), mine(h)]))
    border_ids = [halo_ids.at[pl.ds(side * border, border)] for side in range(2)]
    load_halo = [load((11, 1)[side], (halo_hbm.at[side], border_ids[side])) for side in range(2)]
    load_coarse = load(2, (coarse_hbm, coarse))
    load_edges = load(3, (edges_hbm, edges))
    load_in = load(4, (w_ei_hbm, w_ei))
    load(5, *[(source, vectors.at[i]) for i, source in enumerate(vectors_hbm)])
    load_recv = load(6, (recv_hbm, recv_ids))
    load_send = load(7, (send_hbm, send_ids))
    load_row = load(8, (recv_row_hbm, recv_row))
    load_live = load(9, (live_hbm, live))
    load(10, (w_ni_hbm, w_ni), (w_eo_hbm, w_eo), (w_no_hbm, w_no))

    def remote(source, target, s_sem, r_sem, device):
        return pltpu.make_async_remote_copy(
            src_ref=source, dst_ref=target, send_sem=s_sem, recv_sem=r_sem,
            device_id=device, device_id_type=MESH,
        )

    def slots(index):
        return pl.ds(pl.multiple_of(index * slot, slot), slot)

    def drain(sem, blocks, sent=False):
        ref = table.at[pl.ds(0, blocks // quads)]
        total = remote(ref, ref, sem, sem, {"hidden": near})
        if sent:
            total.wait_send()
        else:
            total.wait_recv()

    chunk = rows // NODE_CHUNKS
    spans = [(i * chunk, chunk) for i in range(NODE_CHUNKS)]
    spans.append((rows + 2 * border, far))
    far_span = NODE_CHUNKS
    unit = border // 8
    pieces = []
    for first, units, route in PIECES:
        for side in (1, 0):
            pieces.append((len(spans), side, first * unit, units * unit, route))
            spans.append((rows + (1 - side) * border + first * unit, units * unit))
    early_group, late_group = NODE_CHUNKS, NODE_CHUNKS + 1
    group = {k: k for k in range(NODE_CHUNKS)}
    group[far_span] = late_group
    for k, side, first, size, route in pieces:
        group[k] = early_group if first + size <= border // 2 else late_group
    sent_rows = [0, 0]
    group_rows = [0] * (NODE_CHUNKS + 2)

    def place(k, column):
        start, size = spans[k]
        return table.at[pl.ds(start, size), mine(column)]

    def to_peer(k, j, column, peer, source=None):
        kind = 0 if k < NODE_CHUNKS else 1
        sent_rows[kind] += spans[k][1]
        if j:
            group_rows[group[k]] += spans[k][1]
        copy = remote(
            place(k, column) if source is None else source, place(k, column),
            ag_send.at[kind], pass_recv.at[group[k]] if j else cross_recv.at[k], {"hidden": peer},
        )
        copy.start()
        return copy

    load_nodes.wait()
    pl.semaphore_wait(barrier, patches - 1 + 3)

    crossed = {}
    for k in range(NODE_CHUNKS):
        crossed[k] = to_peer(k, 0, h, cross)
        to_peer(k, 1, h, near)

    load_coarse.wait()
    for owner in range(patches):
        codes = coarse[owner : owner + 1, :].astype(f32)
        square = jnp.broadcast_to(codes, (slot, slot))
        picked = jnp.where(
            lax.broadcasted_iota(jnp.int32, (slot, slot), 0)
            == lax.broadcasted_iota(jnp.int32, (slot, slot), 1), square, 0.0,
        )
        column = jnp.sum(picked, axis=1, keepdims=True)
        asked[pl.ds(owner * slot, slot), :] = jnp.broadcast_to(column, (slot, LANES)).astype(jnp.int32)
    for step in range(1, patches):
        owner = lax.rem(p + step, patches)
        remote(
            asked.at[slots(owner)], req.at[slots(p)], ask_sem.at[0], ask_sem.at[1], {"patch": owner}
        ).start()
    req[slots(p), :] = asked[slots(p), :]
    others = pl.ds(0, (patches - 1) * slot)

    def spread(column):
        plain.reshape(rows, LANES)[...] = table[pl.ds(0, rows), mine(column)].astype(f32)

    def choose(first, size):
        def step(part, carry):
            base = first + part * GATHER
            for u in range(GATHER):
                picked_rows[base + u] = plain[halo_ids[base + u]]
            return carry

        lax.fori_loop(0, size // GATHER, step, 0)

    def halo_part(target, side, first, size):
        start = side * border + first
        choose(start, size)
        part = pl.ds(start, size)
        target[part, :] = picked_rows.reshape(2 * border, LANES)[part, :].astype(bf16)
        return target.at[part]

    def halo_copy(source, k, side, column, s_sem, r_sem):
        copy = remote(source, place(k, column), s_sem, r_sem, {"patch": after if side else before})
        copy.start()
        return copy

    relayed = [piece for piece in pieces if piece[4] == "x"]
    delayed = [piece for piece in pieces if piece[4] == "y"]
    for side in range(2):
        load_halo[side].wait()
    spread(h)
    halos = {}

    def send_halo(i, piece):
        k, side, first, size, route = piece
        held = halo_part(stage, side, first, size)
        halos[k] = halo_copy(held, k, side, h, halo_send.at[0], halo_recv.at[min(i, len(relayed))])

    for i, piece in enumerate(relayed):
        send_halo(i, piece)
    asks = remote(asked.at[others], req.at[others], ask_sem.at[0], ask_sem.at[1], {"hidden": near})
    asks.wait()
    rep[...] = dot(onehot_of(req[...][:, :1], 0, rows), table[pl.ds(0, rows), mine(h)])
    for step in range(1, patches):
        reader = lax.rem(p + step, patches)
        remote(
            rep.at[slots(reader)], far_in.at[slots(p)], ask_sem.at[2], ask_sem.at[3], {"patch": reader}
        ).start()
    answers = remote(rep.at[others], far_in.at[others], ask_sem.at[2], ask_sem.at[3], {"hidden": near})
    far_in[slots(p), :] = rep[slots(p), :]
    for i, piece in enumerate(delayed):
        send_halo(len(relayed) + i, piece)

    load_edges.wait()
    load_in.wait()
    remote(vectors, vectors, load_sem.at[5], load_sem.at[5], {"hidden": near}).wait_recv()

    def begin(step, carry):
        part = pl.ds(pl.multiple_of(step * block, block), block)
        pre[part, :] = 0.5 * (dot(edges[part, :], w_ei[pl.ds(0, width), :]) + b_ei[...])
        return carry

    lax.fori_loop(0, count // block, begin, 0)

    def forward(k):
        to_peer(k, 2, cross, near)

    def project(start, size, weight, target):
        projected = 0.5 * dot(table[pl.ds(start, size), :], w_ei[pl.ds(weight * width, width), :])
        flat = target.reshape(target.shape[0] * quads, LANES)
        for q in range(quads):
            flat[pl.ds(start * quads + q, size, stride=quads), :] = (
                projected[:, q * LANES : (q + 1) * LANES]
            )

    def own_chunk(k):
        drain(pass_recv.at[k], group_rows[k])
        start, size = spans[k]
        project(start, size, 2, tab_r)
        project(start, size, 1, tab_s)

    def relay(piece):
        k = piece[0]
        halos[k].wait_recv()
        crossed[k] = to_peer(k, 0, h, cross)
        to_peer(k, 1, h, near)

    queue = list(relayed)
    for k in range(NODE_CHUNKS):
        crossed[k].wait_recv()
        forward(k)
        if k == NODE_CHUNKS - 1:
            while queue:
                relay(queue.pop(0))
            spread(cross)
            lates = []
            for i, (j, side, first, size, route) in enumerate(delayed):
                held = halo_part(late_stage, side, first, size)
                lates.append((j, halo_copy(held, j, side, cross, late_send.at[0], late_recv.at[i])))
            answers.wait()
            far_out[...] = far_in[...].astype(bf16)
            crossed[far_span] = to_peer(far_span, 0, h, cross, far_out)
            to_peer(far_span, 1, h, near, far_out)
            keep = pltpu.make_async_copy(far_out, place(far_span, h), own_sem.at[0])
            keep.start()
        if k >= 1:
            for _ in range(2):
                if queue:
                    relay(queue.pop(0))
            own_chunk(k - 1)
    own_chunk(NODE_CHUNKS - 1)
    late_rows = sum(piece[3] for piece in delayed)
    drain(halo_recv.at[len(relayed)], late_rows)
    for piece in delayed:
        to_peer(piece[0], 1, h, near)
    load_recv.wait()
    load_send.wait()

    def pick_receivers(start, size):
        def step(part, carry):
            base = start + part * GATHER
            for u in range(GATHER):
                got_r[base + u] = tab_r[recv_ids[base + u]]
            return carry

        lax.fori_loop(0, size // GATHER, step, 0)

    early = [piece for piece in relayed if group[piece[0]] == early_group]
    parts = max(1, len(early) // 2)
    keep.wait()
    for i in range(parts):
        pick_receivers(i * (count // parts), count // parts)
        for piece in early[2 * i : 2 * i + 2]:
            crossed[piece[0]].wait_recv()
            forward(piece[0])

    def merge(step, carry):
        part = pl.ds(pl.multiple_of(step * block, block), block)
        wide = got_r.reshape(count * quads, LANES)
        for q in range(quads):
            lanes = pl.ds(q * LANES, LANES)
            pre[part, lanes] = (
                pre[part, lanes] + wide[pl.ds(step * block * quads + q, block, stride=quads), :]
            )
        return carry

    lax.fori_loop(0, count // block, merge, 0)
    drain(load_sem.at[10], 4 * width * quads)
    for piece in relayed:
        if group[piece[0]] == late_group:
            crossed[piece[0]].wait_recv()
            forward(piece[0])
    crossed[far_span].wait_recv()
    forward(far_span)
    for j, copy in lates:
        copy.wait_recv()
        forward(j)
    drain(pass_recv.at[early_group], group_rows[early_group])
    for side in range(2):
        project(rows + side * border, border // 2, 1, tab_s)
    drain(pass_recv.at[late_group], group_rows[late_group])
    project(spans[far_span][0], spans[far_span][1], 1, tab_s)
    for side in range(2):
        project(rows + side * border + border // 2, border // 2, 1, tab_s)
    load_live.wait()
    load_row.wait()

    def pick_block(index, first, size):
        for u in range(first, first + size):
            got_s[index % 2][u] = tab_s[send_ids[index * block + u]]

    def pick_first(step, carry):
        for u in range(GATHER):
            got_s[0][step * GATHER + u] = tab_s[send_ids[step * GATHER + u]]
        return carry

    def edge(index):
        part = pl.ds(index * block, block)
        wide_s = got_s[index % 2].reshape(block * quads, LANES)
        total = [
            pre[part, q * LANES : (q + 1) * LANES]
            + wide_s[pl.ds(q, block, stride=quads), :]
            for q in range(quads)
        ]
        active = silu_of_half(jnp.concatenate(total, axis=1)).astype(bf16)
        output = dot(active, w_eo[...]) + b_eo[...]
        update = normalize(output, e_gain[...], e_shift[...])
        position = lax.broadcasted_iota(jnp.int32, (block, 1), 0) + index * block
        message = jnp.where(position < live[0], update, 0.0)
        msg[part, :] = message.astype(bf16)
        edges[part, :] = (edges[part, :].astype(f32) + message).astype(bf16)

    cut = share // 4
    blocks = count // block

    def sums(owner, first, size):
        ids = lax.broadcasted_iota(jnp.int32, (size, count), 0) + (owner * share + first)
        return dot(jnp.where(recv_row[...] == ids, 1.0, 0.0).astype(bf16), msg[...])

    lax.fori_loop(0, block // GATHER, pick_first, 0)
    for index in range(blocks):
        if index + 1 < blocks:
            pick_block(index + 1, 0, block)
        edge(index)

    def give_sums(owner, first, size, target, source, r_sem):
        part = pl.ds(first, size)
        source[part, :] = sums(owner, first, size).astype(bf16)
        copy = remote(source.at[part], target.at[part], rs_send.at[0], r_sem, {"hidden": near})
        copy.start()
        return copy

    to_cross = []

    def cross_sums(first, size, copy):
        part = pl.ds(first, size)
        total = sums(cross, first, size)
        copy.wait_recv()
        give_cross[part, :] = (total + got_far[part, :].astype(f32)).astype(bf16)
        for i in range(first // cut, (first + size) // cut):
            piece = pl.ds(i * cut, cut)
            copy = remote(
                give_cross.at[piece], got_cross.at[piece], rs_send.at[0], rs_recv.at[4 + i],
                {"hidden": cross},
            )
            copy.start()
            to_cross.append(copy)

    shares = ((0, cut), (cut, cut), (2 * cut, share - 2 * cut))
    begun = [give_sums(diag, *shares[i], got_far, give_far, rs_recv.at[i]) for i in range(2)]
    cross_sums(*shares[0], begun[0])
    cross_sums(*shares[1], begun[1])
    begun.append(give_sums(diag, *shares[2], got_far, give_far, rs_recv.at[2]))
    cross_sums(*shares[2], begun[2])
    to_near = give_sums(near, 0, share, got_near, give_near, rs_recv.at[3])
    sums_own[...] = sums(h, 0, share)
    own_rows = pl.ds(pl.multiple_of(h * share, share), share)
    node_pre[...] = dot(table[own_rows, :], w_ni[pl.ds(0, width), :]) + b_ni[...]
    to_near.wait_recv()
    for i in range(4):
        part = pl.ds(i * cut, cut)
        to_cross[i].wait_recv()
        total = sums_own[part, :] + got_near[part, :].astype(f32) + got_cross[part, :].astype(f32)
        inner = node_pre[part, :] + dot(total.astype(bf16), w_ni[pl.ds(width, width), :])
        output = dot(silu_of_half(0.5 * inner).astype(bf16), w_no[...]) + b_no[...]
        update = normalize(output, n_gain[...], n_shift[...])
        spot = pl.ds(pl.multiple_of(h * share + i * cut, cut), cut)
        fresh[part, :] = (table[spot, :].astype(f32) + update).astype(bf16)
        for peer in (cross, diag, near):
            remote(
                fresh.at[part, mine(peer)], nodes_out.at[spot, :],
                out_sem.at[0], out_sem.at[1], {"hidden": peer},
            ).start()
        nodes_out[spot, :] = fresh[part, mine(h)]
    for kind in range(2):
        drain(ag_send.at[kind], sent_rows[kind], True)
    drain(halo_send.at[0], 2 * border, True)
    drain(late_send.at[0], late_rows, True)
    drain(rs_send.at[0], 3 * share * quads, True)
    drain(out_sem.at[0], 3 * share, True)
    drain(out_sem.at[1], 3 * share)


def store(nodes, edges, nodes_out, edges_out, sems):
    size = edges.shape[0] // STORE_PARTS
    copies = [
        pltpu.make_async_copy(
            edges.at[pl.ds(i * size, size)], edges_out.at[pl.ds(i * size, size)], sems.at[i]
        )
        for i in range(STORE_PARTS)
    ]
    copies.append(pltpu.make_async_copy(nodes, nodes_out, sems.at[STORE_PARTS]))
    for copy in copies:
        copy.start()
    for copy in copies:
        copy.wait()


def local(
    nodes, edges, senders, receivers, halo_rows, coarse_rows, edge_count,
    w_edge_in, b_edge_in, w_edge_out, b_edge_out, edge_gain, edge_shift,
    w_node_in, b_node_in, w_node_out, b_node_out, node_gain, node_shift,
    *, patches,
):
    rows, cols = nodes.shape
    count, width = edges.shape
    border = halo_rows.shape[2]
    slot = coarse_rows.shape[2]
    far = patches * slot
    table_rows = rows + 2 * border + far
    share = rows // 4
    block = min(512, count)
    quads = width // LANES
    vmem = pl.BlockSpec(memory_space=pltpu.VMEM)
    hbm = pl.BlockSpec(memory_space=pl.ANY)
    dma = pltpu.SemaphoreType.DMA
    spans = NODE_CHUNKS + 1 + 2 * len(PIECES)
    late = 2 * sum(piece[2] == "y" for piece in PIECES)
    i32 = jnp.int32
    fresh_nodes, fresh_edges = pl.pallas_call(
        functools.partial(kernel, patches, slot, border, block, quads),
        out_shape=(pltpu.VMEM((rows, cols), bf16), pltpu.VMEM((count, width), bf16)),
        in_specs=[hbm] * 20,
        out_specs=(vmem, vmem),
        scratch_shapes=[
            pltpu.VMEM((table_rows, width), bf16),
            pltpu.VMEM((table_rows, quads, LANES), f32),
            pltpu.VMEM((rows, quads, LANES), f32),
            pltpu.VMEM((block, quads, LANES), f32),
            pltpu.VMEM((block, quads, LANES), f32),
            pltpu.VMEM((count, quads, LANES), f32),
            pltpu.VMEM((rows, 1, LANES), f32),
            pltpu.VMEM((2 * border, 1, LANES), f32),
            pltpu.VMEM((2 * border, cols), bf16),
            pltpu.VMEM((2 * border, cols), bf16),
            pltpu.VMEM((patches, slot), i32),
            pltpu.VMEM((far, LANES), i32),
            pltpu.VMEM((far, LANES), i32),
            pltpu.VMEM((far, cols), f32),
            pltpu.VMEM((far, cols), f32),
            pltpu.VMEM((far, cols), bf16),
            pltpu.VMEM((1, count), i32),
            pltpu.VMEM((8, 1, width), f32),
            pltpu.VMEM(w_edge_in.shape, bf16),
            pltpu.VMEM(w_edge_out.shape, bf16),
            pltpu.VMEM(w_node_in.shape, bf16),
            pltpu.VMEM(w_node_out.shape, bf16),
            pltpu.VMEM((count, width), f32),
            pltpu.VMEM((share, width), f32),
            pltpu.VMEM((share, width), f32),
            pltpu.VMEM((count, width), bf16),
            pltpu.SMEM((count,), i32),
            pltpu.SMEM((count,), i32),
            pltpu.SMEM((2 * border,), i32),
            pltpu.SMEM((1,), i32),
        ] + [pltpu.VMEM((share, width), bf16)] * 7 + [
            dma((12,)), dma((1,)), dma((2,)), dma((spans - late,)), dma((NODE_CHUNKS + 2,)),
            dma((1,)), dma((2 * len(PIECES) - late + 1,)), dma((1,)), dma((late,)),
            dma((4,)), dma((1,)), dma((8,)), dma((2,)),
        ],
        compiler_params=pltpu.CompilerParams(
            collective_id=0, has_side_effects=True, vmem_limit_bytes=56 * 1024 * 1024
        ),
    )(
        nodes, halo_rows.reshape(2, border), coarse_rows.reshape(patches, slot),
        edges, w_edge_in, w_edge_out, w_node_in, w_node_out, senders, receivers,
        receivers.reshape(1, -1), edge_count,
        b_edge_in.reshape(1, -1), b_edge_out.reshape(1, -1),
        edge_gain.reshape(1, -1), edge_shift.reshape(1, -1),
        b_node_in.reshape(1, -1), b_node_out.reshape(1, -1),
        node_gain.reshape(1, -1), node_shift.reshape(1, -1),
    )
    return pl.pallas_call(
        store,
        out_shape=(
            jax.ShapeDtypeStruct((rows, cols), bf16), jax.ShapeDtypeStruct((count, width), bf16)
        ),
        in_specs=[vmem] * 2,
        out_specs=(hbm, hbm),
        scratch_shapes=[dma((1 + STORE_PARTS,))],
    )(
        pltpu.with_memory_space_constraint(fresh_nodes, pltpu.VMEM),
        pltpu.with_memory_space_constraint(fresh_edges, pltpu.VMEM),
    )


def solution(mesh):
    spread = P(("patch", "hidden"))
    return jax.shard_map(
        functools.partial(local, patches=mesh.shape["patch"]),
        mesh=mesh,
        in_specs=(
            P("patch", "hidden"), P(("patch", "hidden"), None), spread, spread,
            P("patch", None, None), P("patch", None, None), spread,
        ) + (P(),) * 12,
        out_specs=(P("patch", "hidden"), P(("patch", "hidden"), None)),
        check_vma=False,
    )
```
